32 devices in a mesh: gx: 4 (over x, core), gy: 4 (over z), gz: 2 (over y).
Axes of the slice: x: 2, y: 2, z: 4, core: 2. Of those that a mesh axis runs over, the one named last changes fastest.
Arguments:
- inv_factor: bfloat16 [4, 4, 2, 1536, 1536], P('gx', 'gy', 'gz'), as said below
- coupling: bfloat16 [4, 4, 2, 1536, 1536], P('gx', 'gy', 'gz'), may hold values from -0.15625 to 0.15625
- stiff_gg: bfloat16 [4, 4, 2, 1536, 1536], P('gx', 'gy', 'gz'), as said below
- block_order: int32 [4, 4, 2, 12], P('gx', 'gy', 'gz'), may hold values from 0 to 11, each once within a row
Outputs:
- assembled: float32 [4, 4, 2, 1536, 1536], P('gx', 'gy', 'gz')
The draws below stay inside these ranges and needn't reach their ends.
Inputs may be any that keep to these rules, and one draw needn't show every extreme that they name: `block_order`: each subdomain's row is a permutation of 0 to 11. `stiff_gg`: each subdomain's block is symmetric. `inv_factor`: each subdomain's block is lower triangular with a positive diagonal.
All inputs are finite; a program needn't handle non-finite values.
Results may differ from the reference program's by a relative error of at most 0.0016.
Values sent between devices are 32-bit elements; how exact they have to be, the bound alone decides.
A program may use at most 128 MiB of HBM per device.

```python
import math
import jax
import jax.numpy as jnp
import numpy as np
from jax import lax

NI = 1536
BLK = 128
NBLK = 12
NG = 1536
SUB_X = 4
SUB_Y = 4
SUB_Z = 2


def draw_inv_factor(key, part):
    shape = (SUB_X, SUB_Y, SUB_Z, NI, NI)
    first_key, second_key = jax.random.split(jax.random.fold_in(key, 11))
    entries = jax.random.normal(first_key, shape, jnp.float32)
    lower = jnp.tril(entries, -1) / math.sqrt(NI)
    diagonal = jax.random.uniform(second_key, shape[:-1], jnp.float32, 0.5, 1.5)
    return (lower + diagonal[..., None] * jnp.eye(NI, dtype=jnp.float32)).astype(jnp.bfloat16)


def draw_stiff_gg(key, part):
    shape = (SUB_X, SUB_Y, SUB_Z, NG, NG)
    first_key, second_key = jax.random.split(jax.random.fold_in(key, 23))
    base = jax.random.normal(first_key, shape, jnp.float32)
    symmetric = (base + jnp.swapaxes(base, -1, -2)) / math.sqrt(2.0 * NG)
    diagonal = jax.random.uniform(second_key, shape[:-1], jnp.float32, 2.0, 4.0)
    return (symmetric + diagonal[..., None] * jnp.eye(NG, dtype=jnp.float32)).astype(jnp.bfloat16)


def block_levels(rng, shape, shards, smallest, top_value):
    gain, own = 1.0, jax.random.fold_in(rng, 6)
    for position, parts in shards:
        steps = jnp.exp(jax.random.uniform(jax.random.fold_in(own, position), (parts,), jnp.float32, smallest / len(shards), top_value / len(shards)))
        gain = gain * jnp.repeat(steps, shape[position] // parts).reshape([-1 if axis == position else 1 for axis in range(len(shape))])
    return gain


def bell_draw(rng, shape, scale, limit, cuts=(), kind=jnp.bfloat16):
    values = jax.random.normal(rng, shape, jnp.float32) * scale
    if len(cuts) > 0:
        values = block_levels(rng, shape, cuts, -0.22, 0.18) * values
    return jnp.clip(values, min=-limit, max=limit).astype(kind)


def setup_inputs(seed: int = 0) -> dict:
    keys = jax.random.split(jax.random.key(seed), 5)
    return {
        "inv_factor": draw_inv_factor(jax.random.fold_in(keys[4], 71), 0),
        "coupling": bell_draw(keys[1], (SUB_X, SUB_Y, SUB_Z, NI, NG), NI ** -0.5, 0.15625, ((0, 4), (1, 4), (2, 2))),
        "stiff_gg": draw_stiff_gg(jax.random.fold_in(keys[4], 71), 0),
        "block_order": jax.vmap(lambda own: jax.random.permutation(own, NBLK))(jax.random.split(keys[3], SUB_X * SUB_Y * SUB_Z)).reshape((SUB_X, SUB_Y, SUB_Z, NBLK)).astype(jnp.int32),
    }


west_blocks = (0,)
east_blocks = (1,)
south_blocks = (2, 8, 10)
north_blocks = (3, 9, 11)
bottom_blocks = (4, 5, 8, 9)
top_blocks = (6, 7, 10, 11)


def local_tile(operands):
    inverse, coupled, stiffness = operands
    weighted = jnp.dot(inverse, coupled, preferred_element_type=jnp.float32).astype(jnp.bfloat16)
    product = jnp.dot(weighted.T, weighted, preferred_element_type=jnp.float32)
    return stiffness.astype(jnp.float32) - product


def reorder(matrix, ranking):
    return matrix[ranking][:, ranking]


def shifted(values, axis, direction):
    extent = values.shape[axis]
    zeros_edge = jnp.zeros_like(lax.slice_in_dim(values, 0, 1, axis=axis))
    if direction > 0:
        return jnp.concatenate([zeros_edge, lax.slice_in_dim(values, 0, extent - 1, axis=axis)], axis)
    return jnp.concatenate([lax.slice_in_dim(values, 1, extent, axis=axis), zeros_edge], axis)


def section_sum(grid, axis, lower_list, upper_list):
    lower_idx = np.array(lower_list, dtype=np.int32)
    upper_idx = np.array(upper_list, dtype=np.int32)
    lower_piece = grid[:, :, :, lower_idx][:, :, :, :, lower_idx]
    upper_piece = grid[:, :, :, upper_idx][:, :, :, :, upper_idx]
    from_lower = shifted(upper_piece, axis, 1)
    from_upper = shifted(lower_piece, axis, -1)
    grid = grid.at[:, :, :, lower_idx[:, None], lower_idx[None, :]].add(from_lower)
    grid = grid.at[:, :, :, upper_idx[:, None], upper_idx[None, :]].add(from_upper)
    return grid


def reference(inv_factor, coupling, stiff_gg, block_order):
    total = SUB_X * SUB_Y * SUB_Z
    tiles = lax.map(local_tile, (inv_factor.reshape(total, NI, NI), coupling.reshape(total, NI, NG), stiff_gg.reshape(total, NG, NG)))
    blocked = tiles.reshape(total, NBLK, BLK, NBLK, BLK).transpose(0, 1, 3, 2, 4)
    ranks = block_order.reshape(total, NBLK).astype(jnp.int32)
    canonical = jax.vmap(reorder)(blocked, ranks)
    grid = canonical.reshape(SUB_X, SUB_Y, SUB_Z, NBLK, NBLK, BLK, BLK)
    grid = section_sum(grid, 0, west_blocks, east_blocks)
    grid = section_sum(grid, 1, south_blocks, north_blocks)
    grid = section_sum(grid, 2, bottom_blocks, top_blocks)
    inverse_rank = jnp.argsort(ranks, axis=1).astype(jnp.int32)
    own = jax.vmap(reorder)(grid.reshape(total, NBLK, NBLK, BLK, BLK), inverse_rank)
    return own.transpose(0, 1, 3, 2, 4).reshape(SUB_X, SUB_Y, SUB_Z, NG, NG)
```

```python
import functools

import jax
import jax.numpy as jnp
from jax import lax
from jax.experimental import pallas as pl
from jax.experimental.pallas import tpu as pltpu
from jax.sharding import PartitionSpec as P

HIGH_FIRST = (6, 7, 10, 11, 4, 5, 8, 9, 0, 1, 2, 3)
LOW_FIRST = (4, 5, 8, 9, 6, 7, 10, 11, 0, 1, 2, 3)
WEST, EAST = 8, 9
SOUTH, NORTH = (10, 2, 6), (11, 3, 7)
PANEL = 4
PANELS = 3
Z_PAIRS = ((0, 0), (0, 1), (0, 2), (0, 3), (1, 1), (1, 2), (1, 3), (2, 3), (2, 2), (3, 3))
Z_RUNS = ((0, 0, 4, 0), (1, 1, 3, 4), (2, 3, 1, 7), (2, 2, 1, 8), (3, 3, 1, 9))
Z_EARLY = 3
Y_PAIRS = ((1, 1), (2, 2), (0, 0), (0, 1), (0, 2), (1, 2))
MESH = pl.DeviceIdType.MESH


class Side:
    def __init__(self, axis):
        size = lax.axis_size(axis)
        self.axis = axis
        self.at = lax.axis_index(axis)
        self.lower = self.at > 0
        self.upper = self.at < size - 1
        self.size = size

    def toward(self, step):
        return {self.axis: self.at + step}


def slot_rank(order_ref, has_upper, slot):
    return jnp.where(has_upper, order_ref[HIGH_FIRST[slot]], order_ref[LOW_FIRST[slot]])


def weigh_part(inv_part, coupled, weighted, flipped, part):
    rows = inv_part.shape[0]
    here = pl.ds(part * rows, rows)
    product = jnp.dot(
        inv_part[...], coupled[pl.ds(0, (part + 1) * rows), :], preferred_element_type=jnp.float32
    ).astype(weighted.dtype)
    weighted[here, :] = product
    flipped[:, here] = product.T


def begin_kernel(
    order_ref, inv_hbm, coup_hbm, stiff_hbm,
    inv_0, inv_1, inv_2, coupled, stiff, weighted, flipped, tile, sems,
):
    inv_parts = (inv_0, inv_1, inv_2)
    parts = len(inv_parts)
    rows = inv_0.shape[0]
    slots, _, blk, _ = stiff.shape
    wide = PANEL * blk
    at = lax.axis_index("gz")
    has_upper = at < lax.axis_size("gz") - 1
    ranks = [slot_rank(order_ref, has_upper, slot) for slot in range(slots)]

    def span(slot):
        return pl.ds(pl.multiple_of(ranks[slot] * blk, blk), blk)

    def load_stiff(a, b, sem):
        pltpu.make_async_copy(stiff_hbm.at[span(a), span(b)], stiff.at[a, b], sem).start()

    for part in range(parts):
        here = pl.ds(part * rows, rows)
        for slot in range(PANEL):
            pltpu.make_async_copy(
                coup_hbm.at[here, span(slot)], coupled.at[here, pl.ds(slot * blk, blk)], sems.at[part]
            ).start()
        pltpu.make_async_copy(
            inv_hbm.at[here, pl.ds(0, (part + 1) * rows)], inv_parts[part], sems.at[parts + part]
        ).start()
    for a in range(PANEL):
        for b in range(PANEL):
            load_stiff(a, b, sems.at[2 * parts])
    for slot in range(PANEL, slots):
        pltpu.make_async_copy(
            coup_hbm.at[:, span(slot)], coupled.at[:, pl.ds(slot * blk, blk)], sems.at[2 * parts + 1]
        ).start()
    for a in range(PANEL):
        for b in range(PANEL, slots):
            load_stiff(a, b, sems.at[2 * parts + 2])
    for a in range(PANEL, slots):
        for b in range(slots):
            load_stiff(a, b, sems.at[2 * parts + 3])

    def arrived(ref, sem):
        pltpu.make_async_copy(ref, ref, sem).wait()

    panel = coupled.at[:, pl.ds(0, wide)]
    for part in range(parts):
        arrived(coupled.at[pl.ds(part * rows, rows), pl.ds(0, wide)], sems.at[part])
        arrived(inv_parts[part], sems.at[parts + part])
        weigh_part(inv_parts[part], panel, weighted, flipped, part)
    arrived(stiff.at[pl.ds(0, PANEL), pl.ds(0, PANEL)], sems.at[2 * parts])
    product = jnp.dot(flipped[...], weighted[...], preferred_element_type=jnp.float32)
    for a in range(PANEL):
        for b in range(PANEL):
            tile[a, b] = stiff[a, b].astype(jnp.float32) - product[
                a * blk : (a + 1) * blk, b * blk : (b + 1) * blk
            ]
    arrived(coupled.at[:, pl.ds(wide, (slots - PANEL) * blk)], sems.at[2 * parts + 1])
    arrived(stiff.at[pl.ds(0, PANEL), pl.ds(PANEL, slots - PANEL)], sems.at[2 * parts + 2])
    arrived(stiff.at[pl.ds(PANEL, slots - PANEL)], sems.at[2 * parts + 3])


def assemble_kernel(
    inv_0, inv_1, inv_2, coupled, stiff, weighted_0, flipped_0, tile_0, tile,
    weighted_1, weighted_2, flipped_1, flipped_2,
    got_x, got_y, got_z, x_send, x_recv, y_send, y_recv, z_send, z_recv,
):
    inv_parts = (inv_0, inv_1, inv_2)
    weighted = (weighted_0, weighted_1, weighted_2)
    flipped = (flipped_0, flipped_1, flipped_2)
    blk = tile.shape[-1]
    wide = PANEL * blk
    parts = len(inv_parts)
    gx, gy, gz = Side("gx"), Side("gy"), Side("gz")

    barrier = pltpu.get_barrier_semaphore()
    for side in (gx, gy, gz):
        @pl.when(side.lower)
        def _(side=side):
            pl.semaphore_signal(barrier, inc=1, device_id=side.toward(-1), device_id_type=MESH)

        @pl.when(side.upper)
        def _(side=side):
            pl.semaphore_signal(barrier, inc=1, device_id=side.toward(1), device_id_type=MESH)

    def weigh(panel, part):
        columns = coupled.at[:, pl.ds(panel * wide, wide)]
        weigh_part(inv_parts[part], columns, weighted[panel], flipped[panel], part)

    def multiply(first, second):
        product = jnp.dot(
            flipped[first][...], weighted[second][...], preferred_element_type=jnp.float32
        )
        for row in range(PANEL):
            for col in range(PANEL):
                a, b = first * PANEL + row, second * PANEL + col
                tile[a, b] = stiff[a, b].astype(jnp.float32) - product[
                    row * blk : (row + 1) * blk, col * blk : (col + 1) * blk
                ]

    def y_copy(number, up):
        mine, way = (NORTH, 1) if up else (SOUTH, 0)
        first, second = Y_PAIRS[number]
        return pltpu.make_async_remote_copy(
            src_ref=(tile_0 if number == 0 else tile).at[mine[first], mine[second]],
            dst_ref=got_y.at[1 - way, number],
            send_sem=y_send.at[way, number],
            recv_sem=y_recv.at[1 - way, number],
            device_id=gy.toward(1 if up else -1),
            device_id_type=MESH,
        )

    def y_arrival(number, from_lower):
        place = 0 if from_lower else 1
        return pltpu.make_async_remote_copy(
            src_ref=got_y.at[place, number],
            dst_ref=got_y.at[place, number],
            send_sem=y_send.at[1 - place, number],
            recv_sem=y_recv.at[place, number],
            device_id=gy.toward(-1 if from_lower else 1),
            device_id_type=MESH,
        )

    def y_start(numbers):
        @pl.when(gy.lower)
        def _():
            for number in numbers:
                y_copy(number, False).start()

        @pl.when(gy.upper)
        def _():
            for number in numbers:
                y_copy(number, True).start()

    def add_pair(a, b, value):
        tile[a, b] = tile[a, b] + value
        if a != b:
            tile[b, a] = tile[b, a] + value.T

    def y_finish(numbers):
        for has, mine, place, up in ((gy.lower, SOUTH, 0, False), (gy.upper, NORTH, 1, True)):
            @pl.when(has)
            def _(mine=mine, place=place, up=up):
                for number in numbers:
                    first, second = Y_PAIRS[number]
                    y_copy(number, up).wait_send()
                    y_arrival(number, place == 0).wait_recv()
                    add_pair(mine[first], mine[second], got_y[place, number])

    z_first = gz.lower | gz.upper
    z_both = gz.lower & gz.upper

    def z_copy(panel, run):
        row, col, count, place = Z_RUNS[run]
        if panel == 0:
            target = gz.at + jnp.where(gz.upper, 1, -1)
            kind = jnp.where(target < gz.size - 1, jnp.where(gz.upper, 1, 0), 0)
        else:
            target = gz.at - 1
            kind = 0
        return pltpu.make_async_remote_copy(
            src_ref=(tile_0 if panel == 0 and run < Z_EARLY else tile).at[
                panel * PANEL + row, pl.ds(panel * PANEL + col, count)
            ],
            dst_ref=got_z.at[kind, pl.ds(place, count)],
            send_sem=z_send.at[panel, run],
            recv_sem=z_recv.at[kind, run],
            device_id={"gz": target},
            device_id_type=MESH,
        )

    def z_start(panel, runs):
        @pl.when(z_first if panel == 0 else z_both)
        def _():
            for run in runs:
                z_copy(panel, run).start()

    def z_finish(panel):
        @pl.when(z_first if panel == 0 else z_both)
        def _():
            for run, (_, _, count, place) in enumerate(Z_RUNS):
                z_copy(panel, run).wait_send()
                pltpu.make_async_remote_copy(
                    src_ref=got_z.at[panel, pl.ds(place, count)],
                    dst_ref=got_z.at[panel, pl.ds(place, count)],
                    send_sem=z_send.at[panel, run],
                    recv_sem=z_recv.at[panel, run],
                    device_id={"gz": gz.at + (jnp.where(gz.upper, 1, -1) if panel == 0 else -1)},
                    device_id_type=MESH,
                ).wait_recv()
            for number, (row, col) in enumerate(Z_PAIRS):
                add_pair(panel * PANEL + row, panel * PANEL + col, got_z[panel, number])

    def x_copy(up):
        way, slot = (1, EAST) if up else (0, WEST)
        return pltpu.make_async_remote_copy(
            src_ref=tile.at[slot, slot],
            dst_ref=got_x.at[1 - way],
            send_sem=x_send.at[way],
            recv_sem=x_recv.at[1 - way],
            device_id=gx.toward(1 if up else -1),
            device_id_type=MESH,
        )

    def x_start():
        @pl.when(gx.lower)
        def _():
            x_copy(False).start()

        @pl.when(gx.upper)
        def _():
            x_copy(True).start()

    def x_finish():
        for has, slot, place, up in ((gx.lower, WEST, 0, False), (gx.upper, EAST, 1, True)):
            @pl.when(has)
            def _(slot=slot, place=place, up=up):
                x_copy(up).wait_send()
                pltpu.make_async_remote_copy(
                    src_ref=got_x.at[place],
                    dst_ref=got_x.at[place],
                    send_sem=x_send.at[1 - place],
                    recv_sem=x_recv.at[place],
                    device_id=gx.toward(1 if up else -1),
                    device_id_type=MESH,
                ).wait_recv()
                tile[slot, slot] = tile[slot, slot] + got_x[place]

    weigh(1, 0)
    neighbours = sum(
        side.lower.astype(jnp.int32) + side.upper.astype(jnp.int32) for side in (gx, gy, gz)
    )
    pl.semaphore_wait(barrier, neighbours)
    y_start((0,))
    z_start(0, range(Z_EARLY))
    tile[0:PANEL, 0:PANEL] = tile_0[...]
    for part in range(1, parts):
        weigh(1, part)
    multiply(1, 1)
    weigh(2, 0)
    y_start((1,))
    z_start(1, range(Z_EARLY))
    y_finish((0,))
    weigh(2, 1)
    z_start(0, range(Z_EARLY, len(Z_RUNS)))
    y_finish((1,))
    weigh(2, 2)
    z_start(1, range(Z_EARLY, len(Z_RUNS)))
    multiply(2, 2)
    multiply(2, 0)
    x_start()
    y_start((2, 3))
    multiply(2, 1)
    y_start((4,))
    multiply(0, 1)
    y_start((5,))
    multiply(1, 0)
    multiply(0, 2)
    multiply(1, 2)
    x_finish()
    y_finish((2, 3, 4, 5))
    z_finish(1)
    z_finish(0)


def place_kernel(order_ref, tile, out_hbm, sem):
    slots, _, blk, _ = tile.shape
    at = lax.axis_index("gz")
    has_upper = at < lax.axis_size("gz") - 1
    ranks = [slot_rank(order_ref, has_upper, slot) for slot in range(slots)]
    for a in range(slots):
        for b in range(slots):
            pltpu.make_async_copy(
                tile.at[a, b],
                out_hbm.at[
                    pl.ds(pl.multiple_of(ranks[a] * blk, blk), blk),
                    pl.ds(pl.multiple_of(ranks[b] * blk, blk), blk),
                ],
                sem,
            ).start()
    pltpu.make_async_copy(out_hbm, out_hbm, sem).wait()


def shards(inv_factor, coupling, stiff_gg, block_order):
    order = block_order.reshape(block_order.shape[-1:])
    inverse, coupled, stiffness = inv_factor[0, 0, 0], coupling[0, 0, 0], stiff_gg[0, 0, 0]
    slots = order.shape[0]
    inner, outer = coupled.shape
    blk = outer // slots
    parts = 3
    rows = inner // parts
    narrow = coupled.dtype
    smem = pl.BlockSpec(memory_space=pltpu.SMEM)
    vmem = pl.BlockSpec(memory_space=pltpu.VMEM)
    hbm = pl.BlockSpec(memory_space=pltpu.HBM)
    wide = PANEL * blk
    held = pl.pallas_call(
        begin_kernel,
        out_shape=[pltpu.VMEM((rows, (part + 1) * rows), narrow) for part in range(parts)]
        + [
            pltpu.VMEM((inner, outer), narrow),
            pltpu.VMEM((slots, slots, blk, blk), narrow),
            pltpu.VMEM((inner, wide), narrow),
            pltpu.VMEM((wide, inner), narrow),
            pltpu.VMEM((PANEL, PANEL, blk, blk), jnp.float32),
        ],
        in_specs=[smem, hbm, hbm, hbm],
        out_specs=[vmem] * (parts + 5),
        scratch_shapes=[pltpu.SemaphoreType.DMA((2 * parts + 4,))],
        compiler_params=pltpu.CompilerParams(vmem_limit_bytes=43 * 1024 * 1024),
        name="begin",
    )(order, inverse, coupled, stiffness)
    tile = pl.pallas_call(
        assemble_kernel,
        out_shape=pltpu.VMEM((slots, slots, blk, blk), jnp.float32),
        in_specs=[vmem] * (parts + 5),
        out_specs=vmem,
        scratch_shapes=[pltpu.VMEM((inner, wide), narrow)] * (PANELS - 1)
        + [pltpu.VMEM((wide, inner), narrow)] * (PANELS - 1)
        + [
            pltpu.VMEM((2, blk, blk), jnp.float32),
            pltpu.VMEM((2, len(Y_PAIRS), blk, blk), jnp.float32),
            pltpu.VMEM((2, len(Z_PAIRS), blk, blk), jnp.float32),
            pltpu.SemaphoreType.DMA((2,)),
            pltpu.SemaphoreType.DMA((2,)),
            pltpu.SemaphoreType.DMA((2, len(Y_PAIRS))),
            pltpu.SemaphoreType.DMA((2, len(Y_PAIRS))),
            pltpu.SemaphoreType.DMA((2, len(Z_RUNS))),
            pltpu.SemaphoreType.DMA((2, len(Z_RUNS))),
        ],
        compiler_params=pltpu.CompilerParams(
            collective_id=0, has_side_effects=True, vmem_limit_bytes=16 * 1024 * 1024
        ),
        name="assemble",
    )(*held)
    own = pl.pallas_call(
        place_kernel,
        out_shape=jax.ShapeDtypeStruct((outer, outer), jnp.float32),
        in_specs=[smem, pl.BlockSpec(memory_space=pl.ANY)],
        out_specs=hbm,
        scratch_shapes=[pltpu.SemaphoreType.DMA],
        compiler_params=pltpu.CompilerParams(vmem_limit_bytes=1024 * 1024),
        name="place",
    )(order, tile)
    return own.reshape(1, 1, 1, outer, outer)


def solution(mesh):
    return jax.shard_map(
        shards,
        mesh=mesh,
        in_specs=(
            P("gx", "gy", "gz", None, None),
            P("gx", "gy", "gz", None, None),
            P("gx", "gy", "gz", None, None),
            P("gx", "gy", "gz", None),
        ),
        out_specs=P("gx", "gy", "gz", None, None),
        check_vma=False,
    )
```

```python
import functools

import jax
import jax.numpy as jnp
from jax import lax
from jax.experimental import pallas as pl
from jax.experimental.pallas import tpu as pltpu
from jax.sharding import PartitionSpec as P

HIGH_FIRST = (6, 7, 10, 11, 4, 5, 8, 9, 0, 1, 2, 3)
LOW_FIRST = (4, 5, 8, 9, 6, 7, 10, 11, 0, 1, 2, 3)
WEST, EAST = 8, 9
SOUTH, NORTH = (10, 2, 6), (11, 3, 7)
PANEL = 4
PANELS = 3
Z_PAIRS = ((0, 0), (0, 1), (0, 2), (0, 3), (1, 1), (1, 2), (1, 3), (2, 3), (2, 2), (3, 3))
Z_RUNS = ((0, 0, 4, 0), (1, 1, 3, 4), (2, 3, 1, 7), (2, 2, 1, 8), (3, 3, 1, 9))
Z_EARLY = 3
Y_PAIRS = ((1, 1), (2, 2), (0, 0), (0, 1), (0, 2), (1, 2))
MESH = pl.DeviceIdType.MESH


class Side:
    def __init__(self, axis):
        size = lax.axis_size(axis)
        self.axis = axis
        self.at = lax.axis_index(axis)
        self.lower = self.at > 0
        self.upper = self.at < size - 1
        self.size = size

    def toward(self, step):
        return {self.axis: self.at + step}


def slot_rank(order_ref, has_upper, slot):
    return jnp.where(has_upper, order_ref[HIGH_FIRST[slot]], order_ref[LOW_FIRST[slot]])


def weigh_part(inv_part, coupled, weighted, flipped, part):
    rows = inv_part.shape[0]
    here = pl.ds(part * rows, rows)
    product = jnp.dot(
        inv_part[...], coupled[pl.ds(0, (part + 1) * rows), :], preferred_element_type=jnp.float32
    ).astype(weighted.dtype)
    weighted[here, :] = product
    flipped[:, here] = product.T


def begin_kernel(
    order_ref, inv_hbm, coup_hbm, stiff_hbm,
    inv_0, inv_1, inv_2, coupled, stiff, weighted, flipped, tile, sems,
):
    inv_parts = (inv_0, inv_1, inv_2)
    parts = len(inv_parts)
    rows = inv_0.shape[0]
    slots, _, blk, _ = stiff.shape
    wide = PANEL * blk
    at = lax.axis_index("gz")
    has_upper = at < lax.axis_size("gz") - 1
    ranks = [slot_rank(order_ref, has_upper, slot) for slot in range(slots)]

    def span(slot):
        return pl.ds(pl.multiple_of(ranks[slot] * blk, blk), blk)

    def load_stiff(a, b, sem):
        pltpu.make_async_copy(stiff_hbm.at[span(a), span(b)], stiff.at[a, b], sem).start()

    for part in range(parts):
        here = pl.ds(part * rows, rows)
        for slot in range(PANEL):
            pltpu.make_async_copy(
                coup_hbm.at[here, span(slot)], coupled.at[here, pl.ds(slot * blk, blk)], sems.at[part]
            ).start()
        pltpu.make_async_copy(
            inv_hbm.at[here, pl.ds(0, (part + 1) * rows)], inv_parts[part], sems.at[parts + part]
        ).start()
    for a in range(PANEL):
        for b in range(PANEL):
            load_stiff(a, b, sems.at[2 * parts])
    for slot in range(PANEL, slots):
        pltpu.make_async_copy(
            coup_hbm.at[:, span(slot)], coupled.at[:, pl.ds(slot * blk, blk)], sems.at[2 * parts + 1]
        ).start()
    for a in range(PANEL):
        for b in range(PANEL, slots):
            load_stiff(a, b, sems.at[2 * parts + 2])
    for a in range(PANEL, slots):
        for b in range(slots):
            load_stiff(a, b, sems.at[2 * parts + 3])

    def arrived(ref, sem):
        pltpu.make_async_copy(ref, ref, sem).wait()

    panel = coupled.at[:, pl.ds(0, wide)]
    for part in range(parts):
        arrived(coupled.at[pl.ds(part * rows, rows), pl.ds(0, wide)], sems.at[part])
        arrived(inv_parts[part], sems.at[parts + part])
        weigh_part(inv_parts[part], panel, weighted, flipped, part)
    arrived(stiff.at[pl.ds(0, PANEL), pl.ds(0, PANEL)], sems.at[2 * parts])
    product = jnp.dot(flipped[...], weighted[...], preferred_element_type=jnp.float32)
    for a in range(PANEL):
        for b in range(PANEL):
            tile[a, b] = stiff[a, b].astype(jnp.float32) - product[
                a * blk : (a + 1) * blk, b * blk : (b + 1) * blk
            ]
    arrived(coupled.at[:, pl.ds(wide, (slots - PANEL) * blk)], sems.at[2 * parts + 1])
    arrived(stiff.at[pl.ds(0, PANEL), pl.ds(PANEL, slots - PANEL)], sems.at[2 * parts + 2])
    arrived(stiff.at[pl.ds(PANEL, slots - PANEL)], sems.at[2 * parts + 3])


def assemble_kernel(
    inv_0, inv_1, inv_2, coupled, stiff, weighted_0, flipped_0, tile_0, tile,
    weighted_1, weighted_2, flipped_1, flipped_2,
    got_x, got_y, got_z, x_send, x_recv, y_send, y_recv, z_send, z_recv,
):
    inv_parts = (inv_0, inv_1, inv_2)
    weighted = (weighted_0, weighted_1, weighted_2)
    flipped = (flipped_0, flipped_1, flipped_2)
    blk = tile.shape[-1]
    wide = PANEL * blk
    parts = len(inv_parts)
    gx, gy, gz = Side("gx"), Side("gy"), Side("gz")

    barrier = pltpu.get_barrier_semaphore()
    for side in (gx, gy, gz):
        @pl.when(side.lower)
        def _(side=side):
            pl.semaphore_signal(barrier, inc=1, device_id=side.toward(-1), device_id_type=MESH)

        @pl.when(side.upper)
        def _(side=side):
            pl.semaphore_signal(barrier, inc=1, device_id=side.toward(1), device_id_type=MESH)

    def weigh(panel, part):
        columns = coupled.at[:, pl.ds(panel * wide, wide)]
        weigh_part(inv_parts[part], columns, weighted[panel], flipped[panel], part)

    def multiply(first, second):
        product = jnp.dot(
            flipped[first][...], weighted[second][...], preferred_element_type=jnp.float32
        )
        for row in range(PANEL):
            for col in range(PANEL):
                a, b = first * PANEL + row, second * PANEL + col
                tile[a, b] = stiff[a, b].astype(jnp.float32) - product[
                    row * blk : (row + 1) * blk, col * blk : (col + 1) * blk
                ]

    def y_copy(number, up):
        mine, way = (NORTH, 1) if up else (SOUTH, 0)
        first, second = Y_PAIRS[number]
        return pltpu.make_async_remote_copy(
            src_ref=(tile_0 if number == 0 else tile).at[mine[first], mine[second]],
            dst_ref=got_y.at[1 - way, number],
            send_sem=y_send.at[way, number],
            recv_sem=y_recv.at[1 - way, number],
            device_id=gy.toward(1 if up else -1),
            device_id_type=MESH,
        )

    def y_arrival(number, from_lower):
        place = 0 if from_lower else 1
        return pltpu.make_async_remote_copy(
            src_ref=got_y.at[place, number],
            dst_ref=got_y.at[place, number],
            send_sem=y_send.at[1 - place, number],
            recv_sem=y_recv.at[place, number],
            device_id=gy.toward(-1 if from_lower else 1),
            device_id_type=MESH,
        )

    def y_start(numbers):
        @pl.when(gy.lower)
        def _():
            for number in numbers:
                y_copy(number, False).start()

        @pl.when(gy.upper)
        def _():
            for number in numbers:
                y_copy(number, True).start()

    def add_pair(a, b, value):
        tile[a, b] = tile[a, b] + value
        if a != b:
            tile[b, a] = tile[b, a] + value.T

    def y_finish(numbers):
        for has, mine, place, up in ((gy.lower, SOUTH, 0, False), (gy.upper, NORTH, 1, True)):
            @pl.when(has)
            def _(mine=mine, place=place, up=up):
                for number in numbers:
                    first, second = Y_PAIRS[number]
                    y_copy(number, up).wait_send()
                    y_arrival(number, place == 0).wait_recv()
                    add_pair(mine[first], mine[second], got_y[place, number])

    z_first = gz.lower | gz.upper
    z_both = gz.lower & gz.upper

    def z_copy(panel, run):
        row, col, count, place = Z_RUNS[run]
        if panel == 0:
            target = gz.at + jnp.where(gz.upper, 1, -1)
            kind = jnp.where(target < gz.size - 1, jnp.where(gz.upper, 1, 0), 0)
        else:
            target = gz.at - 1
            kind = 0
        return pltpu.make_async_remote_copy(
            src_ref=(tile_0 if panel == 0 and run < Z_EARLY else tile).at[
                panel * PANEL + row, pl.ds(panel * PANEL + col, count)
            ],
            dst_ref=got_z.at[kind, pl.ds(place, count)],
            send_sem=z_send.at[panel, run],
            recv_sem=z_recv.at[kind, run],
            device_id={"gz": target},
            device_id_type=MESH,
        )

    def z_start(panel, runs):
        @pl.when(z_first if panel == 0 else z_both)
        def _():
            for run in runs:
                z_copy(panel, run).start()

    def z_finish(panel):
        @pl.when(z_first if panel == 0 else z_both)
        def _():
            for run, (_, _, count, place) in enumerate(Z_RUNS):
                z_copy(panel, run).wait_send()
                pltpu.make_async_remote_copy(
                    src_ref=got_z.at[panel, pl.ds(place, count)],
                    dst_ref=got_z.at[panel, pl.ds(place, count)],
                    send_sem=z_send.at[panel, run],
                    recv_sem=z_recv.at[panel, run],
                    device_id={"gz": gz.at + (jnp.where(gz.upper, 1, -1) if panel == 0 else -1)},
                    device_id_type=MESH,
                ).wait_recv()
            for number, (row, col) in enumerate(Z_PAIRS):
                add_pair(panel * PANEL + row, panel * PANEL + col, got_z[panel, number])

    def x_copy(up):
        way, slot = (1, EAST) if up else (0, WEST)
        return pltpu.make_async_remote_copy(
            src_ref=tile.at[slot, slot],
            dst_ref=got_x.at[1 - way],
            send_sem=x_send.at[way],
            recv_sem=x_recv.at[1 - way],
            device_id=gx.toward(1 if up else -1),
            device_id_type=MESH,
        )

    def x_start():
        @pl.when(gx.lower)
        def _():
            x_copy(False).start()

        @pl.when(gx.upper)
        def _():
            x_copy(True).start()

    def x_finish():
        for has, slot, place, up in ((gx.lower, WEST, 0, False), (gx.upper, EAST, 1, True)):
            @pl.when(has)
            def _(slot=slot, place=place, up=up):
                x_copy(up).wait_send()
                pltpu.make_async_remote_copy(
                    src_ref=got_x.at[place],
                    dst_ref=got_x.at[place],
                    send_sem=x_send.at[1 - place],
                    recv_sem=x_recv.at[place],
                    device_id=gx.toward(1 if up else -1),
                    device_id_type=MESH,
                ).wait_recv()
                tile[slot, slot] = tile[slot, slot] + got_x[place]

    weigh(2, 0)
    neighbours = sum(
        side.lower.astype(jnp.int32) + side.upper.astype(jnp.int32) for side in (gx, gy, gz)
    )
    pl.semaphore_wait(barrier, neighbours)
    y_start((0,))
    z_start(0, range(Z_EARLY))
    tile[0:PANEL, 0:PANEL] = tile_0[...]
    weigh(2, 1)
    weigh(2, 2)
    multiply(2, 2)
    y_finish((0,))
    x_start()
    y_start((2,))
    multiply(2, 0)
    z_start(0, range(Z_EARLY, len(Z_RUNS)))
    y_start((3,))
    for part in range(parts):
        weigh(1, part)
    multiply(1, 1)
    y_start((1,))
    z_start(1, range(Z_EARLY))
    multiply(0, 1)
    y_start((5,))
    multiply(2, 1)
    y_start((4,))
    multiply(1, 0)
    y_finish((1,))
    multiply(0, 2)
    z_start(1, range(Z_EARLY, len(Z_RUNS)))
    multiply(1, 2)
    x_finish()
    y_finish((2, 3, 4, 5))
    z_finish(1)
    z_finish(0)


def place_kernel(order_ref, tile, out_hbm, sem):
    slots, _, blk, _ = tile.shape
    at = lax.axis_index("gz")
    has_upper = at < lax.axis_size("gz") - 1
    ranks = [slot_rank(order_ref, has_upper, slot) for slot in range(slots)]
    for a in range(slots):
        for b in range(slots):
            pltpu.make_async_copy(
                tile.at[a, b],
                out_hbm.at[
                    pl.ds(pl.multiple_of(ranks[a] * blk, blk), blk),
                    pl.ds(pl.multiple_of(ranks[b] * blk, blk), blk),
                ],
                sem,
            ).start()
    pltpu.make_async_copy(out_hbm, out_hbm, sem).wait()


def shards(inv_factor, coupling, stiff_gg, block_order):
    order = block_order.reshape(block_order.shape[-1:])
    inverse, coupled, stiffness = inv_factor[0, 0, 0], coupling[0, 0, 0], stiff_gg[0, 0, 0]
    slots = order.shape[0]
    inner, outer = coupled.shape
    blk = outer // slots
    parts = 3
    rows = inner // parts
    narrow = coupled.dtype
    smem = pl.BlockSpec(memory_space=pltpu.SMEM)
    vmem = pl.BlockSpec(memory_space=pltpu.VMEM)
    hbm = pl.BlockSpec(memory_space=pltpu.HBM)
    wide = PANEL * blk
    held = pl.pallas_call(
        begin_kernel,
        out_shape=[pltpu.VMEM((rows, (part + 1) * rows), narrow) for part in range(parts)]
        + [
            pltpu.VMEM((inner, outer), narrow),
            pltpu.VMEM((slots, slots, blk, blk), narrow),
            pltpu.VMEM((inner, wide), narrow),
            pltpu.VMEM((wide, inner), narrow),
            pltpu.VMEM((PANEL, PANEL, blk, blk), jnp.float32),
        ],
        in_specs=[smem, hbm, hbm, hbm],
        out_specs=[vmem] * (parts + 5),
        scratch_shapes=[pltpu.SemaphoreType.DMA((2 * parts + 4,))],
        compiler_params=pltpu.CompilerParams(vmem_limit_bytes=43 * 1024 * 1024),
        name="begin",
    )(order, inverse, coupled, stiffness)
    tile = pl.pallas_call(
        assemble_kernel,
        out_shape=pltpu.VMEM((slots, slots, blk, blk), jnp.float32),
        in_specs=[vmem] * (parts + 5),
        out_specs=vmem,
        scratch_shapes=[pltpu.VMEM((inner, wide), narrow)] * (PANELS - 1)
        + [pltpu.VMEM((wide, inner), narrow)] * (PANELS - 1)
        + [
            pltpu.VMEM((2, blk, blk), jnp.float32),
            pltpu.VMEM((2, len(Y_PAIRS), blk, blk), jnp.float32),
            pltpu.VMEM((2, len(Z_PAIRS), blk, blk), jnp.float32),
            pltpu.SemaphoreType.DMA((2,)),
            pltpu.SemaphoreType.DMA((2,)),
            pltpu.SemaphoreType.DMA((2, len(Y_PAIRS))),
            pltpu.SemaphoreType.DMA((2, len(Y_PAIRS))),
            pltpu.SemaphoreType.DMA((2, len(Z_RUNS))),
            pltpu.SemaphoreType.DMA((2, len(Z_RUNS))),
        ],
        compiler_params=pltpu.CompilerParams(
            collective_id=0, has_side_effects=True, vmem_limit_bytes=16 * 1024 * 1024
        ),
        name="assemble",
    )(*held)
    own = pl.pallas_call(
        place_kernel,
        out_shape=jax.ShapeDtypeStruct((outer, outer), jnp.float32),
        in_specs=[smem, pl.BlockSpec(memory_space=pl.ANY)],
        out_specs=hbm,
        scratch_shapes=[pltpu.SemaphoreType.DMA],
        compiler_params=pltpu.CompilerParams(vmem_limit_bytes=1024 * 1024),
        name="place",
    )(order, tile)
    return own.reshape(1, 1, 1, outer, outer)


def solution(mesh):
    return jax.shard_map(
        shards,
        mesh=mesh,
        in_specs=(
            P("gx", "gy", "gz", None, None),
            P("gx", "gy", "gz", None, None),
            P("gx", "gy", "gz", None, None),
            P("gx", "gy", "gz", None),
        ),
        out_specs=P("gx", "gy", "gz", None, None),
        check_vma=False,
    )
```
